256 devices in a mesh: freq: 128 (over x, z, y_hi, core), row: 2 (over y_lo).
Axes of the slice: x: 4, y: 4 (y_hi: 2, y_lo: 2; y = y_hi * 2 + y_lo), z: 8, core: 2. Of those that a mesh axis runs over, the one named last changes fastest.
Arguments:
- reflect_re: float32 [128, 1728, 1728], P('freq', 'row'), may hold values from -0.046875 to 0.046875
- reflect_im: float32 [128, 1728, 1728], P('freq', 'row'), may hold values from -0.046875 to 0.046875
- focus_re: float32 [128, 1728, 32], P('freq', 'row'), may hold values from -6 to 6
- focus_im: float32 [128, 1728, 32], P('freq', 'row'), may hold values from -6 to 6
- first_arrival: int32 [1728, 32], P('row'), may hold values from 32 to 127
Outputs:
- minus_re: float32 [128, 1728, 32], P('freq', 'row')
- minus_im: float32 [128, 1728, 32], P('freq', 'row')
- plus_re: float32 [128, 1728, 32], P('freq', 'row')
- plus_im: float32 [128, 1728, 32], P('freq', 'row')
The draws below stay inside these ranges and needn't reach their ends.
All inputs are finite; a program needn't handle non-finite values.
Results may differ from the reference program's by a relative error of at most 0.0001.
Values sent between devices are 32-bit elements; how exact they have to be, the bound alone decides.
A program may use at most 128 MiB of HBM per device.

```python
import math
import jax
import jax.numpy as jnp
from jax import lax

NR = 1728
NP = 32
ITERS = 4
NF = 128
NT = 256


def with_ends(result, key, smallest, top_value):
    index_at = [jax.random.randint(jax.random.fold_in(key, axis), (), 0, length) for axis, length in enumerate(result.shape)]
    widest = result.shape.index(max(result.shape))
    next_to = index_at[:widest] + [(index_at[widest] + 1) % result.shape[widest]] + index_at[widest + 1:]
    return result.at[tuple(index_at)].set(smallest).at[tuple(next_to)].set(top_value)


def block_scale(key, dims, split, least, top_value):
    loudness, own = 1.0, jax.random.fold_in(key, 6)
    for position, parts in split:
        draws = jnp.exp(jax.random.uniform(jax.random.fold_in(own, position), (parts,), jnp.float32, least / len(split), top_value / len(split)))
        loudness = loudness * jnp.repeat(draws, dims[position] // parts).reshape([-1 if axis == position else 1 for axis in range(len(dims))])
    return loudness


def gaussian(own_key, extent, width, bound, split=(), held_as=jnp.bfloat16):
    entries = width * jax.random.normal(own_key, extent, jnp.float32)
    if split:
        entries = entries * block_scale(own_key, extent, split, -0.22, 0.18)
    return jnp.clip(entries, -bound, bound).astype(held_as)


def setup_inputs(seed: int = 0) -> dict:
    splits = jax.random.split(jax.random.key(seed), 6)
    reflect_re = gaussian(splits[0], (NF, NR, NR), (11 * NR) ** -0.5, 0.046875, ((0, 128), (1, 2)), jnp.float32)
    reflect_im = gaussian(splits[1], (NF, NR, NR), (11 * NR) ** -0.5, 0.046875, ((0, 128), (1, 2)), jnp.float32)
    focus_re = gaussian(splits[2], (NF, NR, NP), 1.0, 6.0, ((0, 128), (1, 2)), jnp.float32)
    focus_im = gaussian(splits[3], (NF, NR, NP), 1.0, 6.0, ((0, 128), (1, 2)), jnp.float32)
    first_arrival = with_ends(jax.random.randint(splits[4], (NR, NP), NT // 8, NT // 2), jax.random.fold_in(splits[4], 1), NT // 8, (NT // 2) - 1).astype(jnp.int32)
    return {"reflect_re": reflect_re, "reflect_im": reflect_im, "focus_re": focus_re, "focus_im": focus_im, "first_arrival": first_arrival}


def spectra(freq_count, time_count):
    freq_ids = jnp.arange(freq_count, dtype=jnp.int32)
    time_ids = jnp.arange(time_count, dtype=jnp.int32)
    phase_ids = (time_ids[:, None] * freq_ids[None, :]) % time_count
    angle = (2.0 * math.pi / time_count) * phase_ids.astype(jnp.float32)
    weight = jnp.where(freq_ids == 0, 1.0 / time_count, 2.0 / time_count).astype(jnp.float32)
    return jnp.cos(angle), jnp.sin(angle), weight


def reference(reflect_re, reflect_im, focus_re, focus_im, first_arrival):
    highest = lax.Precision.HIGHEST
    cosine, sine, weight = spectra(NF, NT)
    time_ids = jnp.arange(NT, dtype=jnp.int32)
    distance = jnp.minimum(time_ids, NT - time_ids)
    window = (distance[:, None, None] < first_arrival[None, :, :]).astype(jnp.float32)

    def apply(field_re, field_im, conjugate):
        first = jnp.einsum('fij,fjp->fip', reflect_re, field_re, precision=highest)
        second = jnp.einsum('fij,fjp->fip', reflect_im, field_im, precision=highest)
        third = jnp.einsum('fij,fjp->fip', reflect_re, field_im, precision=highest)
        fourth = jnp.einsum('fij,fjp->fip', reflect_im, field_re, precision=highest)
        if conjugate:
            return first + second, third - fourth
        return first - second, third + fourth

    def filtered(spec_re, spec_im):
        traces = jnp.einsum('tk,kip->tip', cosine * weight[None, :], spec_re, precision=highest)
        traces = traces - jnp.einsum('tk,kip->tip', sine * weight[None, :], spec_im, precision=highest)
        masked = traces * window
        out_re = jnp.einsum('tk,tip->kip', cosine, masked, precision=highest)
        out_im = -jnp.einsum('tk,tip->kip', sine, masked, precision=highest)
        return out_re, out_im

    plus_re, plus_im = focus_re, focus_im
    minus_re = jnp.zeros_like(focus_re)
    minus_im = jnp.zeros_like(focus_im)
    for section in range(ITERS):
        if section % 2 == 0:
            minus_re, minus_im = filtered(*apply(plus_re, plus_im, False))
        else:
            upd_re, upd_im = filtered(*apply(minus_re, minus_im, True))
            plus_re = focus_re + upd_re
            plus_im = focus_im + upd_im
    return minus_re, minus_im, plus_re, plus_im
```

```python
import functools
import math

import jax
import jax.numpy as jnp
import numpy as np
from jax import lax
from jax.experimental import pallas as pl
from jax.experimental.pallas import tpu as pltpu
from jax.sharding import PartitionSpec as P

MESH = pl.DeviceIdType.MESH
ITERS = 4
F32 = jnp.float32
BF16 = jnp.bfloat16
BLK = 216
CHUNK = 96


def split_np(table):
    hi = table.astype(jnp.bfloat16)
    lo = (table - hi.astype(np.float64)).astype(hi.dtype)
    return hi, lo


def tables():
    order = np.array(
        [
            x * 32 + z * 4 + y * 2 + c
            for z in range(8)
            for x in range(4)
            for y in range(2)
            for c in range(2)
        ]
    )
    t = np.arange(256)
    angle = 2.0 * math.pi * ((t[:, None] * order[None, :]) % 256) / 256
    weight = np.where(order == 0, 1.0 / 256, 2.0 / 256)
    t1 = np.concatenate([np.cos(angle) * weight, -np.sin(angle) * weight], axis=1)
    t2 = np.concatenate([np.cos(angle).T, -np.sin(angle).T], axis=0)
    out = []
    for table in (t1, t2):
        hi, lo = split_np(table)
        out.append(np.concatenate([hi, lo, hi], axis=1))
    return out


def split(v):
    hi = v.astype(BF16)
    lo = (v - hi.astype(F32)).astype(BF16)
    return hi, lo


def copies(src, dst, ssem, rsem, dev):
    return pltpu.make_async_remote_copy(
        src_ref=src, dst_ref=dst, send_sem=ssem, recv_sem=rsem, device_id=dev, device_id_type=MESH
    )


def wait_bytes(ref, sem):
    pltpu.make_async_copy(ref, ref, sem).wait()


def kernel(
    rre, rim, fre, fim, fa, t1, t2,
    mre, mim, pre, pim,
    stage, rcat, acc, fsend, relay1, gbuf, bsend, relay2, urecv, fasend, farecv,
    ld_sem, ini_send, ini_recv, fa_send, fa_recv,
    f1_send, f1_recv, f2_send, f2_recv, b1_send, b1_recv, b2_send, b2_send2, b2_recv,
):
    me = lax.axis_index("freq")
    row = lax.axis_index("row")
    x = me // 32
    z = (me // 4) % 8
    yh = (me // 2) % 2
    c = me % 2
    ypos = 2 * yh + row
    xs = [lax.rem(x + d, 4) for d in range(4)]
    zs = [lax.rem(z + d, 8) for d in range(8)]
    ys = [lax.rem(ypos + d, 4) for d in range(4)]
    cs = [c, 1 - c]

    def dev(xi, zi, yi, ci):
        return (xi * 32 + zi * 4 + (yi // 2) * 2 + ci, lax.rem(yi, 2))

    plane = [(dx, dy, dc) for dx in (2, 1, 3, 0) for dy in (2, 1, 3, 0) for dc in (1, 0)][:-1]
    zorder = [4, 3, 5, 2, 6, 1, 7]
    barrier = pltpu.get_barrier_semaphore()
    for dx, dy, dc in plane:
        pl.semaphore_signal(
            barrier, inc=1, device_id=dev(xs[dx], z, ys[dy], cs[dc]), device_id_type=MESH
        )
    for dz in zorder:
        pl.semaphore_signal(barrier, inc=1, device_id=dev(x, zs[dz], ypos, c), device_id_type=MESH)

    nchunk = rre.shape[0] // CHUNK
    for k in range(nchunk):
        for a, ref in enumerate((rre, rim)):
            pltpu.make_async_copy(
                ref.at[pl.ds(k * CHUNK, CHUNK)],
                stage.at[a, pl.ds(k * CHUNK, CHUNK)],
                ld_sem.at[k, a],
            ).start()

    u2 = urecv.reshape(5 * 8 * 128, 128)
    for q in range(4):
        base = (row * 4 + q) * 128
        for h in range(2):
            n = 128 if h == 0 else BLK - 128
            rows = pl.ds(BLK * q + 128 * h, n)
            both = jnp.concatenate([fre[rows, :], fim[rows, :], jnp.zeros((n, 64), F32)], axis=1)
            if n < 128:
                both = jnp.concatenate([both, jnp.zeros((128 - n, 128), F32)], axis=0)
            both = both.T
            for ri in range(2):
                u2[pl.ds(base + 2 * h + ri, 32, stride=4), :] = both[32 * ri : 32 * ri + 32]
    myq = 2 * yh + c
    myp = x * 8 + z
    pick = lax.broadcasted_iota(jnp.int32, (128, 128), 0) == myp
    for h in range(2):
        n = 128 if h == 0 else BLK - 128
        rows = pl.ds(pl.multiple_of(BLK * myq + 128 * h, 8), n)
        v = jnp.concatenate([fa[rows, :].astype(F32), jnp.zeros((n, 96), F32)], axis=1)
        if n < 128:
            v = jnp.concatenate([v, jnp.zeros((128 - n, 128), F32)], axis=0)
        v = jnp.sum(jnp.where(pick, v.T, 0.0), axis=0, keepdims=True)
        fasend[8 * h : 8 * h + 8] = jnp.broadcast_to(v, (8, 128))

    pl.semaphore_wait(barrier, len(plane) + len(zorder))
    partner = (me, 1 - row)
    mine = urecv.at[0, pl.ds(row * 4, 4)]
    ini = copies(mine, mine, ini_send, ini_recv, partner)
    ini.start()
    fac = copies(fasend, farecv, fa_send, fa_recv, partner)
    fac.start()

    def convert(k, carry):
        rows = pl.ds(pl.multiple_of(k * CHUNK, CHUNK), CHUNK)
        for a in range(2):
            wait_bytes(stage.at[a, pl.ds(0, CHUNK)], ld_sem.at[k, a])
            for b in range(8):
                v = stage[a, rows, BLK * b : BLK * b + BLK]
                v = jnp.concatenate([v, jnp.zeros((CHUNK, 256 - BLK), F32)], axis=1)
                hi, lo = split(v)
                rcat[b, rows, 512 * a : 512 * a + 256] = hi
                rcat[b, rows, 512 * a + 256 : 512 * a + 512] = lo
        return carry

    lax.fori_loop(0, nchunk, convert, 0)
    acc[864:, :] = jnp.zeros_like(acc[864:, :])
    ini.wait()
    fac.wait()

    f1v = fsend.reshape(ITERS * 512, 128)
    g2 = gbuf.reshape(ITERS * 512, 128)
    bs2 = bsend.reshape(ITERS * 512, 128)
    ublk = urecv.reshape(5 * 32, 8, 4, 128)
    sid = (x * 2 + yh) * 2 + c
    myn = (1 - row) * 4 + myq
    reach = jnp.concatenate([farecv[0:1], farecv[8:9]], axis=1)
    tid = lax.broadcasted_iota(jnp.int32, (256, 256), 0)
    dist = jnp.minimum(tid, 256 - tid).astype(F32)

    def apply(it, carry):
        sign = 1.0 - 2.0 * lax.rem(it, 2).astype(F32)
        extra = jnp.where(it == 2, 1.0, 0.0).astype(F32)

        def block(dy, dc, first):
            yi = lax.rem(ypos + dy, 4)
            ci = lax.rem(c + dc, 2)
            n = (1 - lax.rem(yi, 2)) * 4 + (yi // 2) * 2 + ci

            @pl.when(it > 0)
            def _():
                if first:
                    wait_bytes(urecv.at[it, n, pl.ds(0, 3)], b2_recv.at[it, n])
                else:
                    wait_bytes(urecv.at[it, n], b2_recv.at[it, n])

            parts = []
            for ri in range(2):
                halves = []
                for h in range(2):
                    j = 2 * h + ri
                    now = u2[pl.ds((it * 8 + n) * 128 + j, 32, stride=4), :]
                    start = u2[pl.ds(n * 128 + j, 32, stride=4), :]
                    halves.append(now + extra * start)
                parts.append(jnp.concatenate(halves, axis=1))
            ur, ui = parts
            urh, url = split(ur)
            uih, uil = split(ui)
            sg = sign.astype(BF16)
            w1 = jnp.concatenate([urh, uih, url, uil], axis=0)
            w2 = jnp.concatenate([-(sg * uih), sg * urh, -(sg * uil), sg * url], axis=0)
            w = jnp.concatenate([w1, w1, w2, w2], axis=1)
            part = lax.dot_general(
                rcat[n], w, (((1,), (1,)), ((), ())), preferred_element_type=F32
            )
            if first:
                acc[0:864, :] = part
            else:
                acc[0:864, :] += part

        block(0, 0, True)

        def rest(t, carry):
            v = t // 2
            dy = v + v // 2 - 2 * (v // 3)
            block(dy, lax.rem(t, 2), False)
            return carry

        lax.fori_loop(1, 8, rest, 0)

        for q in range(4):
            for h in range(2):
                v = acc[BLK * q + 128 * h : BLK * q + 128 * h + 128, :].T
                v = v[0:64] + v[64:128]
                for ri in range(2):
                    f1v[pl.ds(it * 512 + q * 128 + 2 * h + ri, 32, stride=4), :] = v[
                        32 * ri : 32 * ri + 32
                    ]
            for dx in (2, 1, 3, 0):
                copies(
                    fsend.at[it, q, xs[dx]],
                    relay1.at[it, sid],
                    f1_send.at[it],
                    f1_recv.at[it],
                    dev(xs[dx], z, 2 * (q // 2) + 1 - row, q % 2),
                ).start()
        wait_bytes(relay1.at[it], f1_recv.at[it])
        for dz in zorder:
            copies(
                relay1.at[it, :, zs[dz]],
                gbuf.at[it, z],
                f2_send.at[it],
                f2_recv.at[it],
                dev(x, zs[dz], ypos, c),
            ).start()
        gbuf[it, z] = relay1[it, :, z]
        wait_bytes(gbuf.at[it, pl.ds(0, 7)], f2_recv.at[it])

        g = jnp.concatenate(
            [
                jnp.concatenate(
                    [g2[pl.ds(it * 512 + 2 * h + ri, 128, stride=4), :] for h in range(2)], axis=1
                )
                for ri in range(2)
            ],
            axis=0,
        )
        gh, gl = split(g)
        tr = jnp.dot(t1[...], jnp.concatenate([gh, gh, gl], axis=0), preferred_element_type=F32)
        tr = jnp.where(dist < reach, tr, 0.0)
        th, tl = split(tr)
        out = jnp.dot(t2[...], jnp.concatenate([th, th, tl], axis=0), preferred_element_type=F32)
        for h in range(2):
            for ri in range(2):
                bs2[pl.ds(it * 512 + 2 * h + ri, 128, stride=4), :] = out[
                    128 * ri : 128 * ri + 128, 128 * h : 128 * h + 128
                ]
        for dz in zorder:
            copies(
                bsend.at[it, zs[dz]],
                relay2.at[it, z],
                b1_send.at[it],
                b1_recv.at[it],
                dev(x, zs[dz], ypos, c),
            ).start()
        relay2[it, z] = bsend[it, z]
        wait_bytes(relay2.at[it, pl.ds(0, 7)], b1_recv.at[it])

        def out_to(dx, dy, dc, sem):
            yi = ys[dy]
            s = (xs[dx] * 2 + yi // 2) * 2 + cs[dc]
            copies(
                relay2.at[it, :, s],
                urecv.at[it + 1, myn, x],
                sem,
                b2_recv.at[it + 1, myn],
                dev(xs[dx], z, yi, cs[dc]),
            ).start()

        for dx, dy, dc in plane:
            if dy % 2 == 1:
                out_to(dx, dy, dc, b2_send.at[it])

        @pl.when(it < ITERS - 1)
        def _():
            for dx, dy, dc in plane:
                if dy % 2 == 0:
                    out_to(dx, dy, dc, b2_send2.at[it])
            urecv[it + 1, myn, x] = relay2[it, :, sid]

        wait_bytes(fsend.at[it], f1_send.at[it])
        wait_bytes(gbuf.at[it, pl.ds(0, 7)], f2_send.at[it])
        wait_bytes(relay2.at[it, pl.ds(0, 7)], b1_send.at[it])
        wait_bytes(ublk.at[pl.ds(0, 16)], b2_send.at[it])

        @pl.when(it < ITERS - 1)
        def _():
            wait_bytes(ublk.at[pl.ds(0, 15)], b2_send2.at[it])

        return carry

    lax.fori_loop(0, ITERS, apply, 0)

    for q in range(4):
        n = row * 4 + q
        wait_bytes(urecv.at[ITERS, n], b2_recv.at[ITERS, n])
        for slot, outs in ((ITERS - 1, (mre, mim)), (ITERS, (pre, pim))):
            for h in range(2):
                m = 128 if h == 0 else BLK - 128
                vals = []
                for ri in range(2):
                    j = 2 * h + ri
                    v = u2[pl.ds((slot * 8 + n) * 128 + j, 32, stride=4), :]
                    if slot == ITERS:
                        v = v + u2[pl.ds(n * 128 + j, 32, stride=4), :]
                    vals.append(v)
                vals.append(jnp.zeros((64, 128), F32))
                v = jnp.concatenate(vals, axis=0).T
                rows = pl.ds(BLK * q + 128 * h, m)
                outs[0][rows, :] = v[0:m, 0:32]
                outs[1][rows, :] = v[0:m, 32:64]


def local(reflect_re, reflect_im, focus_re, focus_im, first_arrival):
    rows, cols = reflect_re.shape[1:]
    t1, t2 = tables()
    vmem = pl.BlockSpec(memory_space=pltpu.VMEM)
    hbm = pl.BlockSpec(memory_space=pl.ANY)
    dma = pltpu.SemaphoreType.DMA
    outs = pl.pallas_call(
        kernel,
        out_shape=[jax.ShapeDtypeStruct((rows, 32), F32)] * 4,
        in_specs=[hbm, hbm] + [vmem] * 5,
        out_specs=[vmem] * 4,
        scratch_shapes=[
            pltpu.VMEM((2, rows, cols), F32),
            pltpu.VMEM((8, rows, 1024), BF16),
            pltpu.VMEM((rows + 48, 128), F32),
            pltpu.VMEM((ITERS, 4, 4, 8, 4, 128), F32),
            pltpu.VMEM((ITERS, 16, 8, 4, 128), F32),
            pltpu.VMEM((ITERS, 8, 16, 4, 128), F32),
            pltpu.VMEM((ITERS, 8, 16, 4, 128), F32),
            pltpu.VMEM((ITERS, 8, 16, 4, 128), F32),
            pltpu.VMEM((5, 8, 4, 8, 4, 128), F32),
            pltpu.VMEM((16, 128), F32),
            pltpu.VMEM((16, 128), F32),
            dma((rows // CHUNK, 2)),
            dma, dma, dma, dma,
            dma((ITERS,)), dma((ITERS,)), dma((ITERS,)), dma((ITERS,)),
            dma((ITERS,)), dma((ITERS,)), dma((ITERS,)), dma((ITERS,)),
            dma((5, 8)),
        ],
        compiler_params=pltpu.CompilerParams(
            collective_id=0, has_side_effects=True, vmem_limit_bytes=60 * 1024 * 1024
        ),
    )(
        reflect_re[0], reflect_im[0], focus_re[0], focus_im[0], first_arrival,
        jnp.asarray(t1), jnp.asarray(t2),
    )
    return tuple(o[None] for o in outs)


def solution(mesh):
    placed = (
        P("freq", "row", None),
        P("freq", "row", None),
        P("freq", "row", None),
        P("freq", "row", None),
        P("row", None),
    )
    return jax.shard_map(
        local,
        mesh=mesh,
        in_specs=placed,
        out_specs=(P("freq", "row", None),) * 4,
        check_vma=False,
    )
```

```python
import functools
import math

import jax
import jax.numpy as jnp
import numpy as np
from jax import lax
from jax.experimental import pallas as pl
from jax.experimental.pallas import tpu as pltpu
from jax.sharding import PartitionSpec as P

MESH = pl.DeviceIdType.MESH
ITERS = 4
F32 = jnp.float32
BF16 = jnp.bfloat16
BLK = 216
CHUNK = 96


def split_np(table):
    hi = table.astype(jnp.bfloat16)
    lo = (table - hi.astype(np.float64)).astype(hi.dtype)
    return hi, lo


def tables():
    order = np.array(
        [
            x * 32 + z * 4 + y * 2 + c
            for z in range(8)
            for y in range(2)
            for x in range(4)
            for c in range(2)
        ]
    )
    t = np.arange(256)
    angle = 2.0 * math.pi * ((t[:, None] * order[None, :]) % 256) / 256
    weight = np.where(order == 0, 1.0 / 256, 2.0 / 256)
    t1 = np.concatenate([np.cos(angle) * weight, -np.sin(angle) * weight], axis=1)
    t2 = np.concatenate([np.cos(angle).T, -np.sin(angle).T], axis=0)
    out = []
    for table in (t1, t2):
        hi, lo = split_np(table)
        out.append(np.concatenate([hi, lo, hi], axis=1))
    return out


def split(v):
    hi = v.astype(BF16)
    lo = (v - hi.astype(F32)).astype(BF16)
    return hi, lo


def copies(src, dst, ssem, rsem, dev):
    return pltpu.make_async_remote_copy(
        src_ref=src, dst_ref=dst, send_sem=ssem, recv_sem=rsem, device_id=dev, device_id_type=MESH
    )


def wait_bytes(ref, sem):
    pltpu.make_async_copy(ref, ref, sem).wait()


def kernel(
    rre, rim, fre, fim, fa, t1, t2,
    mre, mim, pre, pim,
    stage, rcat, acc, fsend, relay1, gbuf, bsend, relay2, urecv, fasend, farecv,
    ld_sem, ini_send, ini_recv, fa_send, fa_recv,
    f1_send, f1_recv, f2_send, f2_recv, b1_send, b1_recv, b2_send, b2_send2, b2_recv,
):
    me = lax.axis_index("freq")
    row = lax.axis_index("row")
    x = me // 32
    z = (me // 4) % 8
    yh = (me // 2) % 2
    c = me % 2
    ypos = 2 * yh + row
    xs = [lax.rem(x + d, 4) for d in range(4)]
    zs = [lax.rem(z + d, 8) for d in range(8)]
    ys = [lax.rem(ypos + d, 4) for d in range(4)]
    cs = [c, 1 - c]

    def dev(xi, zi, yi, ci):
        return (xi * 32 + zi * 4 + (yi // 2) * 2 + ci, lax.rem(yi, 2))

    plane = [(dx, dy, dc) for dx in (2, 1, 3, 0) for dy in (2, 1, 3, 0) for dc in (1, 0)][:-1]
    zorder = [4, 3, 5, 2, 6, 1, 7]
    barrier = pltpu.get_barrier_semaphore()
    for dx, dy, dc in plane:
        pl.semaphore_signal(
            barrier, inc=1, device_id=dev(xs[dx], z, ys[dy], cs[dc]), device_id_type=MESH
        )
    for dz in zorder:
        pl.semaphore_signal(barrier, inc=1, device_id=dev(x, zs[dz], ypos, c), device_id_type=MESH)

    nchunk = rre.shape[0] // CHUNK
    for k in range(nchunk):
        for a, ref in enumerate((rre, rim)):
            pltpu.make_async_copy(
                ref.at[pl.ds(k * CHUNK, CHUNK)],
                stage.at[a, pl.ds(k * CHUNK, CHUNK)],
                ld_sem.at[k, a],
            ).start()

    u2 = urecv.reshape(5 * 8 * 128, 128)
    for q in range(4):
        base = (row * 4 + q) * 128
        for h in range(2):
            n = 128 if h == 0 else BLK - 128
            lo = BLK * q + 128 * h
            for ri, ref in enumerate((fre, fim)):
                v = ref[:, lo : lo + n]
                if n < 128:
                    v = jnp.concatenate([v, jnp.zeros((32, 128 - n), F32)], axis=1)
                u2[pl.ds(base + 2 * h + ri, 32, stride=4), :] = v
    myq = 2 * yh + c
    myp = x * 8 + z
    pick = lax.broadcasted_iota(jnp.int32, fa.shape, 0) == myp
    v = jnp.sum(jnp.where(pick, fa[...].astype(F32), 0.0), axis=0, keepdims=True)
    w = jnp.zeros((1, BLK), F32)
    for q in range(4):
        w = w + jnp.where(myq == q, v[:, BLK * q : BLK * q + BLK], 0.0)
    w = jnp.concatenate([w, jnp.zeros((1, 256 - BLK), F32)], axis=1)
    for h in range(2):
        fasend[8 * h : 8 * h + 8] = jnp.broadcast_to(w[:, 128 * h : 128 * h + 128], (8, 128))

    pl.semaphore_wait(barrier, len(plane) + len(zorder))
    partner = (me, 1 - row)
    mine = urecv.at[0, pl.ds(row * 4, 4)]
    ini = copies(mine, mine, ini_send, ini_recv, partner)
    ini.start()
    fac = copies(fasend, farecv, fa_send, fa_recv, partner)
    fac.start()

    def convert(k, carry):
        rows = pl.ds(pl.multiple_of(k * CHUNK, CHUNK), CHUNK)
        for a in range(2):
            wait_bytes(stage.at[a, pl.ds(0, CHUNK)], ld_sem.at[k, a])
            for b in range(8):
                v = stage[a, rows, BLK * b : BLK * b + BLK]
                v = jnp.concatenate([v, jnp.zeros((CHUNK, 256 - BLK), F32)], axis=1)
                hi, lo = split(v)
                rcat[b, rows, 512 * a : 512 * a + 256] = hi
                rcat[b, rows, 512 * a + 256 : 512 * a + 512] = lo
        return carry

    lax.fori_loop(0, nchunk, convert, 0)
    acc[864:, :] = jnp.zeros_like(acc[864:, :])
    fac.wait()

    f1v = fsend.reshape(ITERS * 512, 128)
    g2 = gbuf.reshape(ITERS * 512, 128)
    bs2 = bsend.reshape(ITERS * 512, 128)
    ublk = urecv.reshape(5 * 32, 8, 4, 128)
    sid = x * 2 + c
    myn = (1 - row) * 4 + myq
    reach = jnp.concatenate([farecv[0:1], farecv[8:9]], axis=1)
    tid = lax.broadcasted_iota(jnp.int32, (256, 256), 0)
    dist = jnp.minimum(tid, 256 - tid).astype(F32)

    def apply(it, carry):
        sign = 1.0 - 2.0 * lax.rem(it, 2).astype(F32)
        extra = jnp.where(it == 2, 1.0, 0.0).astype(F32)

        def block(t, first):
            v = t // 2
            ci = lax.rem(c + t + 1, 2)
            y_own = 2 * (v % 2) + lax.rem(row + 1 + v // 2, 2)
            y_arr = 2 * lax.rem(yh + 1 + v // 2, 2) + lax.rem(row + 1 + v % 2, 2)
            yi = jnp.where(it == 0, y_own, y_arr)
            n = (1 - lax.rem(yi, 2)) * 4 + (yi // 2) * 2 + ci

            @pl.when((it > 0) & (t < 7))
            def _():
                wait_bytes(urecv.at[it, n], b2_recv.at[it, n])

            @pl.when((it > 0) & (t == 7))
            def _():
                wait_bytes(urecv.at[it, n, pl.ds(0, 3)], b2_recv.at[it, n])

            @pl.when((it == 0) & (t == 4))
            def _():
                ini.wait()

            parts = []
            for ri in range(2):
                halves = []
                for h in range(2):
                    j = 2 * h + ri
                    now = u2[pl.ds((it * 8 + n) * 128 + j, 32, stride=4), :]
                    start = u2[pl.ds(n * 128 + j, 32, stride=4), :]
                    halves.append(now + extra * start)
                parts.append(jnp.concatenate(halves, axis=1))
            ur, ui = parts
            urh, url = split(ur)
            uih, uil = split(ui)
            sg = sign.astype(BF16)
            w1 = jnp.concatenate([urh, uih, url, uil], axis=0)
            w2 = jnp.concatenate([-(sg * uih), sg * urh, -(sg * uil), sg * url], axis=0)
            w = jnp.concatenate([w1, w1, w2, w2], axis=1)
            part = lax.dot_general(
                rcat[n], w, (((1,), (1,)), ((), ())), preferred_element_type=F32
            )
            if first:
                acc[0:864, :] = part
            else:
                acc[0:864, :] += part

        block(jnp.int32(0), True)

        def rest(t, carry):
            block(t, False)
            return carry

        lax.fori_loop(1, 8, rest, 0)

        for dy in (1, 3):
            yi = ys[dy]
            for cd in range(2):
                q = (yi // 2) * 2 + cd
                for h in range(2):
                    v = acc[pl.ds(pl.multiple_of(BLK * q + 128 * h, 8), 128), :].T
                    v = v[0:64] + v[64:128]
                    for ri in range(2):
                        f1v[pl.ds(it * 512 + q * 128 + 2 * h + ri, 32, stride=4), :] = v[
                            32 * ri : 32 * ri + 32
                        ]
                for dx in (2, 1, 3, 0):
                    copies(
                        fsend.at[it, q, xs[dx]],
                        relay1.at[it, yh, sid],
                        f1_send.at[it],
                        f1_recv.at[it, yh],
                        dev(xs[dx], z, yi, cd),
                    ).start()
        for dy in (3, 1):
            v = ys[dy] // 2
            wait_bytes(relay1.at[it, v], f1_recv.at[it, v])
            for dz in zorder:
                copies(
                    relay1.at[it, v, :, zs[dz]],
                    gbuf.at[it, z, v],
                    f2_send.at[it],
                    f2_recv.at[it],
                    dev(x, zs[dz], ypos, c),
                ).start()
            gbuf[it, z, v] = relay1[it, v, :, z]
        wait_bytes(gbuf.at[it, pl.ds(0, 7)], f2_recv.at[it])

        g = jnp.concatenate(
            [
                jnp.concatenate(
                    [g2[pl.ds(it * 512 + 2 * h + ri, 128, stride=4), :] for h in range(2)], axis=1
                )
                for ri in range(2)
            ],
            axis=0,
        )
        gh, gl = split(g)
        tr = jnp.dot(t1[...], jnp.concatenate([gh, gh, gl], axis=0), preferred_element_type=F32)
        tr = jnp.where(dist < reach, tr, 0.0)
        th, tl = split(tr)
        out = jnp.dot(t2[...], jnp.concatenate([th, th, tl], axis=0), preferred_element_type=F32)
        for h in range(2):
            for ri in range(2):
                bs2[pl.ds(it * 512 + 2 * h + ri, 128, stride=4), :] = out[
                    128 * ri : 128 * ri + 128, 128 * h : 128 * h + 128
                ]
        for v in (1 - yh, yh):
            for dz in zorder:
                copies(
                    bsend.at[it, zs[dz], v],
                    relay2.at[it, v, z],
                    b1_send.at[it],
                    b1_recv.at[it, v],
                    dev(x, zs[dz], ypos, c),
                ).start()
            relay2[it, v, z] = bsend[it, z, v]

        def out_to(dx, v, r, dc, sem):
            copies(
                relay2.at[it, v, :, xs[dx] * 2 + cs[dc]],
                urecv.at[it + 1, myn, x],
                sem,
                b2_recv.at[it + 1, myn],
                dev(xs[dx], z, 2 * v + r, cs[dc]),
            ).start()

        for near, v in enumerate((1 - yh, yh)):
            wait_bytes(relay2.at[it, v, pl.ds(0, 7)], b1_recv.at[it, v])
            for dx in (2, 1, 3, 0):
                for dc in (1, 0):
                    out_to(dx, v, 1 - row, dc, b2_send.at[it])

            @pl.when(it < ITERS - 1)
            def _():
                for dx in (2, 1, 3, 0):
                    for dc in (1, 0):
                        if near and dx == 0 and dc == 0:
                            urecv[it + 1, myn, x] = relay2[it, v, :, sid]
                        else:
                            out_to(dx, v, row, dc, b2_send2.at[it])

        wait_bytes(fsend.at[it], f1_send.at[it])
        wait_bytes(gbuf.at[it, pl.ds(0, 7)], f2_send.at[it])
        wait_bytes(gbuf.at[it, pl.ds(0, 7)], b1_send.at[it])
        wait_bytes(ublk.at[pl.ds(0, 16)], b2_send.at[it])

        @pl.when(it < ITERS - 1)
        def _():
            wait_bytes(ublk.at[pl.ds(0, 15)], b2_send2.at[it])

        return carry

    lax.fori_loop(0, ITERS, apply, 0)

    for q in range(4):
        n = row * 4 + q
        wait_bytes(urecv.at[ITERS, n], b2_recv.at[ITERS, n])
        for slot, outs in ((ITERS - 1, (mre, mim)), (ITERS, (pre, pim))):
            for h in range(2):
                m = 128 if h == 0 else BLK - 128
                lo = BLK * q + 128 * h
                for ri in range(2):
                    j = 2 * h + ri
                    v = u2[pl.ds((slot * 8 + n) * 128 + j, 32, stride=4), :]
                    if slot == ITERS:
                        v = v + u2[pl.ds(n * 128 + j, 32, stride=4), :]
                    outs[ri][:, lo : lo + m] = v[:, 0:m]


def local(reflect_re, reflect_im, focus_re, focus_im, first_arrival):
    rows, cols = reflect_re.shape[1:]
    t1, t2 = tables()
    vmem = pl.BlockSpec(memory_space=pltpu.VMEM)
    hbm = pl.BlockSpec(memory_space=pl.ANY)
    dma = pltpu.SemaphoreType.DMA
    outs = pl.pallas_call(
        kernel,
        out_shape=[jax.ShapeDtypeStruct((32, rows), F32)] * 4,
        in_specs=[hbm, hbm] + [vmem] * 5,
        out_specs=[vmem] * 4,
        scratch_shapes=[
            pltpu.VMEM((2, rows, cols), F32),
            pltpu.VMEM((8, rows, 1024), BF16),
            pltpu.VMEM((rows + 48, 128), F32),
            pltpu.VMEM((ITERS, 4, 4, 8, 4, 128), F32),
            pltpu.VMEM((ITERS, 2, 8, 8, 4, 128), F32),
            pltpu.VMEM((ITERS, 8, 2, 8, 4, 128), F32),
            pltpu.VMEM((ITERS, 8, 2, 8, 4, 128), F32),
            pltpu.VMEM((ITERS, 2, 8, 8, 4, 128), F32),
            pltpu.VMEM((5, 8, 4, 8, 4, 128), F32),
            pltpu.VMEM((16, 128), F32),
            pltpu.VMEM((16, 128), F32),
            dma((rows // CHUNK, 2)),
            dma, dma, dma, dma,
            dma((ITERS,)), dma((ITERS, 2)), dma((ITERS,)), dma((ITERS,)),
            dma((ITERS,)), dma((ITERS, 2)), dma((ITERS,)), dma((ITERS,)),
            dma((5, 8)),
        ],
        compiler_params=pltpu.CompilerParams(
            collective_id=0, has_side_effects=True, vmem_limit_bytes=60 * 1024 * 1024
        ),
    )(
        reflect_re[0], reflect_im[0], focus_re[0].T, focus_im[0].T, first_arrival.T,
        jnp.asarray(t1), jnp.asarray(t2),
    )
    return tuple(o.T[None] for o in outs)


def solution(mesh):
    placed = (
        P("freq", "row", None),
        P("freq", "row", None),
        P("freq", "row", None),
        P("freq", "row", None),
        P("row", None),
    )
    return jax.shard_map(
        local,
        mesh=mesh,
        in_specs=placed,
        out_specs=(P("freq", "row", None),) * 4,
        check_vma=False,
    )
```

```python
import functools
import math

import jax
import jax.numpy as jnp
import numpy as np
from jax import lax
from jax.experimental import pallas as pl
from jax.experimental.pallas import tpu as pltpu
from jax.sharding import PartitionSpec as P

MESH = pl.DeviceIdType.MESH
ITERS = 4
F32 = jnp.float32
BF16 = jnp.bfloat16
BLK = 216
CHUNK = 96


def split_np(table):
    hi = table.astype(jnp.bfloat16)
    lo = (table - hi.astype(np.float64)).astype(hi.dtype)
    return hi, lo


def tables():
    order = np.array(
        [
            x * 32 + z * 4 + y * 2 + c
            for z in range(8)
            for y in range(2)
            for x in range(4)
            for c in range(2)
        ]
    )
    t = np.arange(256)
    angle = 2.0 * math.pi * ((t[:, None] * order[None, :]) % 256) / 256
    weight = np.where(order == 0, 1.0 / 256, 2.0 / 256)
    t1 = np.concatenate([np.cos(angle) * weight, -np.sin(angle) * weight], axis=1)
    t2 = np.concatenate([np.cos(angle).T, -np.sin(angle).T], axis=0)
    out = []
    for table in (t1, t2):
        hi, lo = split_np(table)
        out.append(np.concatenate([hi, lo, hi], axis=1))
    return out


def split(v):
    hi = v.astype(BF16)
    lo = (v - hi.astype(F32)).astype(BF16)
    return hi, lo


def copies(src, dst, ssem, rsem, dev):
    return pltpu.make_async_remote_copy(
        src_ref=src, dst_ref=dst, send_sem=ssem, recv_sem=rsem, device_id=dev, device_id_type=MESH
    )


def wait_bytes(ref, sem):
    pltpu.make_async_copy(ref, ref, sem).wait()


def kernel(
    rre, rim, fre_h, fim_h, fa_h, t1_h, t2_h,
    mre, mim, pre, pim,
    stage, fbuf, fa, t1, t2, rcat, acc, fsend, gbuf, bsend, relay2, urecv, fasend, farecv,
    ld_sem, in_sem, ini_send, ini_recv, fa_send, fa_recv,
    f_send, f_recv, b1_send, b1_recv, b2_send, b2_send2, b2_recv,
):
    me = lax.axis_index("freq")
    row = lax.axis_index("row")
    x = me // 32
    z = (me // 4) % 8
    yh = (me // 2) % 2
    c = me % 2
    ypos = 2 * yh + row
    xs = [lax.rem(x + d, 4) for d in range(4)]
    zs = [lax.rem(z + d, 8) for d in range(8)]
    ys = [lax.rem(ypos + d, 4) for d in range(4)]
    cs = [c, 1 - c]

    def dev(xi, zi, yi, ci):
        return (xi * 32 + zi * 4 + (yi // 2) * 2 + ci, lax.rem(yi, 2))

    loads = [
        pltpu.make_async_copy(src, dst, in_sem.at[i])
        for i, (src, dst) in enumerate(
            ((fre_h, fbuf.at[0]), (fim_h, fbuf.at[1]), (fa_h, fa), (t1_h, t1), (t2_h, t2))
        )
    ]
    for load in loads:
        load.start()
    nchunk = rre.shape[0] // CHUNK
    for k in range(nchunk):
        for a, ref in enumerate((rre, rim)):
            pltpu.make_async_copy(
                ref.at[pl.ds(k * CHUNK, CHUNK)],
                stage.at[a, pl.ds(k * CHUNK, CHUNK)],
                ld_sem.at[k, a],
            ).start()

    xorder, zorder = (2, 1, 3, 0), (4, 3, 5, 2, 6, 1, 7)
    away = [
        (dx, dy, dz, dc) for dz in (*zorder, 0) for dx in xorder for dy in (1, 3) for dc in (1, 0)
    ]
    away += [(dx, dy, 0, dc) for dx in xorder for dy in (2, 0) for dc in (1, 0)][:-1]
    away += [(0, 0, dz, 0) for dz in zorder]
    barrier = pltpu.get_barrier_semaphore()
    for dx, dy, dz, dc in away:
        pl.semaphore_signal(
            barrier, inc=1, device_id=dev(xs[dx], zs[dz], ys[dy], cs[dc]), device_id_type=MESH
        )

    u2 = urecv.reshape(5 * 8 * 128, 128)
    for load in loads[:3]:
        load.wait()
    for q in range(4):
        base = (row * 4 + q) * 128
        for h in range(2):
            n = 128 if h == 0 else BLK - 128
            lo = BLK * q + 128 * h
            for ri in range(2):
                v = fbuf[ri, :, lo : lo + n]
                if n < 128:
                    v = jnp.concatenate([v, jnp.zeros((32, 128 - n), F32)], axis=1)
                u2[pl.ds(base + 2 * h + ri, 32, stride=4), :] = v
    myq = 2 * yh + c
    myp = x * 8 + z
    pick = lax.broadcasted_iota(jnp.int32, fa.shape, 0) == myp
    v = jnp.sum(jnp.where(pick, fa[...].astype(F32), 0.0), axis=0, keepdims=True)
    w = jnp.zeros((1, BLK), F32)
    for q in range(4):
        w = w + jnp.where(myq == q, v[:, BLK * q : BLK * q + BLK], 0.0)
    w = jnp.concatenate([w, jnp.zeros((1, 256 - BLK), F32)], axis=1)
    for h in range(2):
        fasend[8 * h : 8 * h + 8] = jnp.broadcast_to(w[:, 128 * h : 128 * h + 128], (8, 128))

    pl.semaphore_wait(barrier, len(away))
    partner = (me, 1 - row)
    mine = urecv.at[0, pl.ds(row * 4, 4)]
    ini = copies(mine, mine, ini_send, ini_recv, partner)
    ini.start()
    fac = copies(fasend, farecv, fa_send, fa_recv, partner)
    fac.start()

    def convert(k, carry):
        rows = pl.ds(pl.multiple_of(k * CHUNK, CHUNK), CHUNK)
        for a in range(2):
            wait_bytes(stage.at[a, pl.ds(0, CHUNK)], ld_sem.at[k, a])
            for b in range(8):
                v = stage[a, rows, BLK * b : BLK * b + BLK]
                v = jnp.concatenate([v, jnp.zeros((CHUNK, 256 - BLK), F32)], axis=1)
                hi, lo = split(v)
                rcat[b, rows, 512 * a : 512 * a + 256] = hi
                rcat[b, rows, 512 * a + 256 : 512 * a + 512] = lo
        return carry

    lax.fori_loop(0, nchunk, convert, 0)
    acc[864:, :] = jnp.zeros_like(acc[864:, :])
    fac.wait()
    for load in loads[3:]:
        load.wait()

    f1v = fsend.reshape(ITERS * 512, 128)
    g2 = gbuf.reshape(ITERS * 512, 128)
    bs2 = bsend.reshape(ITERS * 512, 128)
    ublk = urecv.reshape(5 * 32, 8, 4, 128)
    sid = x * 2 + c
    myn = (1 - row) * 4 + myq
    reach = jnp.concatenate([farecv[0:1], farecv[8:9]], axis=1)
    tid = lax.broadcasted_iota(jnp.int32, (256, 256), 0)
    dist = jnp.minimum(tid, 256 - tid).astype(F32)

    def apply(it, carry):
        sign = 1.0 - 2.0 * lax.rem(it, 2).astype(F32)
        extra = jnp.where(it == 2, 1.0, 0.0).astype(F32)

        def block(t, first):
            v = t // 2
            ci = lax.rem(c + t + 1, 2)
            y_own = 2 * (v % 2) + lax.rem(row + 1 + v // 2, 2)
            y_arr = 2 * lax.rem(yh + 1 + v // 2, 2) + lax.rem(row + 1 + v % 2, 2)
            yi = jnp.where(it == 0, y_own, y_arr)
            n = (1 - lax.rem(yi, 2)) * 4 + (yi // 2) * 2 + ci

            @pl.when((it > 0) & (t < 7))
            def _():
                wait_bytes(urecv.at[it, n], b2_recv.at[it, n])

            @pl.when((it > 0) & (t == 7))
            def _():
                wait_bytes(urecv.at[it, n, pl.ds(0, 3)], b2_recv.at[it, n])

            @pl.when((it == 0) & (t == 4))
            def _():
                ini.wait()

            parts = []
            for ri in range(2):
                halves = []
                for h in range(2):
                    j = 2 * h + ri
                    now = u2[pl.ds((it * 8 + n) * 128 + j, 32, stride=4), :]
                    start = u2[pl.ds(n * 128 + j, 32, stride=4), :]
                    halves.append(now + extra * start)
                parts.append(jnp.concatenate(halves, axis=1))
            ur, ui = parts
            urh, url = split(ur)
            uih, uil = split(ui)
            sg = sign.astype(BF16)
            w1 = jnp.concatenate([urh, uih, url, uil], axis=0)
            w2 = jnp.concatenate([-(sg * uih), sg * urh, -(sg * uil), sg * url], axis=0)
            w = jnp.concatenate([w1, w1, w2, w2], axis=1)
            part = lax.dot_general(
                rcat[n], w, (((1,), (1,)), ((), ())), preferred_element_type=F32
            )
            if first:
                acc[0:864, :] = part
            else:
                acc[0:864, :] += part

        block(jnp.int32(0), True)

        def rest(t, carry):
            block(t, False)
            return carry

        lax.fori_loop(1, 8, rest, 0)

        for dy in (1, 3):
            yi = ys[dy]
            for cd in range(2):
                q = (yi // 2) * 2 + cd
                for h in range(2):
                    v = acc[pl.ds(pl.multiple_of(BLK * q + 128 * h, 8), 128), :].T
                    v = v[0:64] + v[64:128]
                    for ri in range(2):
                        f1v[pl.ds(it * 512 + q * 128 + 2 * h + ri, 32, stride=4), :] = v[
                            32 * ri : 32 * ri + 32
                        ]
                for dz in (*zorder, 0):
                    for dx in xorder:
                        copies(
                            fsend.at[it, q, xs[dx], zs[dz]],
                            gbuf.at[it, z, yh, sid],
                            f_send.at[it],
                            f_recv.at[it],
                            dev(xs[dx], zs[dz], yi, cd),
                        ).start()
        wait_bytes(gbuf.at[it], f_recv.at[it])

        g = jnp.concatenate(
            [
                jnp.concatenate(
                    [g2[pl.ds(it * 512 + 2 * h + ri, 128, stride=4), :] for h in range(2)], axis=1
                )
                for ri in range(2)
            ],
            axis=0,
        )
        gh, gl = split(g)
        tr = jnp.dot(t1[...], jnp.concatenate([gh, gh, gl], axis=0), preferred_element_type=F32)
        tr = jnp.where(dist < reach, tr, 0.0)
        th, tl = split(tr)
        out = jnp.dot(t2[...], jnp.concatenate([th, th, tl], axis=0), preferred_element_type=F32)
        for h in range(2):
            for ri in range(2):
                bs2[pl.ds(it * 512 + 2 * h + ri, 128, stride=4), :] = out[
                    128 * ri : 128 * ri + 128, 128 * h : 128 * h + 128
                ]
        for v in (1 - yh, yh):
            for dz in zorder:
                copies(
                    bsend.at[it, zs[dz], v],
                    relay2.at[it, v, z],
                    b1_send.at[it],
                    b1_recv.at[it, v],
                    dev(x, zs[dz], ypos, c),
                ).start()
            relay2[it, v, z] = bsend[it, z, v]

        def out_to(dx, v, r, dc, sem):
            copies(
                relay2.at[it, v, :, xs[dx] * 2 + cs[dc]],
                urecv.at[it + 1, myn, x],
                sem,
                b2_recv.at[it + 1, myn],
                dev(xs[dx], z, 2 * v + r, cs[dc]),
            ).start()

        for near, v in enumerate((1 - yh, yh)):
            wait_bytes(relay2.at[it, v, pl.ds(0, 7)], b1_recv.at[it, v])
            for dx in xorder:
                for dc in (1, 0):
                    out_to(dx, v, 1 - row, dc, b2_send.at[it])

            @pl.when(it < ITERS - 1)
            def _():
                for dx in xorder:
                    for dc in (1, 0):
                        if near and dx == 0 and dc == 0:
                            urecv[it + 1, myn, x] = relay2[it, v, :, sid]
                        else:
                            out_to(dx, v, row, dc, b2_send2.at[it])

        return carry

    lax.fori_loop(0, ITERS, apply, 0)

    def result(slot, outs):
        for q in range(4):
            n = row * 4 + q
            if slot == ITERS:
                wait_bytes(urecv.at[ITERS, n], b2_recv.at[ITERS, n])
            for h in range(2):
                m = 128 if h == 0 else BLK - 128
                lo = BLK * q + 128 * h
                for ri in range(2):
                    j = 2 * h + ri
                    v = u2[pl.ds((slot * 8 + n) * 128 + j, 32, stride=4), :]
                    if slot == ITERS:
                        v = v + u2[pl.ds(n * 128 + j, 32, stride=4), :]
                    outs[ri][:, lo : lo + m] = v[:, 0:m]

    result(ITERS - 1, (mre, mim))
    for it in range(ITERS):
        wait_bytes(fsend.at[it], f_send.at[it])
        wait_bytes(gbuf.at[it, pl.ds(0, 7)], b1_send.at[it])
        wait_bytes(ublk.at[pl.ds(0, 16)], b2_send.at[it])
        if it < ITERS - 1:
            wait_bytes(ublk.at[pl.ds(0, 15)], b2_send2.at[it])
    result(ITERS, (pre, pim))


def hand_on(*refs):
    for i in range(4):
        refs[4 + i][...] = refs[i][...]


def local(reflect_re, reflect_im, focus_re, focus_im, first_arrival):
    rows, cols = reflect_re.shape[1:]
    t1, t2 = tables()
    vmem = pl.BlockSpec(memory_space=pltpu.VMEM)
    hbm = pl.BlockSpec(memory_space=pl.ANY)
    dma = pltpu.SemaphoreType.DMA
    outs = pl.pallas_call(
        kernel,
        out_shape=[jax.ShapeDtypeStruct((32, rows), F32)] * 4,
        in_specs=[hbm] * 7,
        out_specs=[vmem] * 4,
        scratch_shapes=[
            pltpu.VMEM((2, rows, cols), F32),
            pltpu.VMEM((2, 32, rows), F32),
            pltpu.VMEM((32, rows), jnp.int32),
            pltpu.VMEM(t1.shape, BF16),
            pltpu.VMEM(t2.shape, BF16),
            pltpu.VMEM((8, rows, 1024), BF16),
            pltpu.VMEM((rows + 48, 128), F32),
            pltpu.VMEM((ITERS, 4, 4, 8, 4, 128), F32),
            pltpu.VMEM((ITERS, 8, 2, 8, 4, 128), F32),
            pltpu.VMEM((ITERS, 8, 2, 8, 4, 128), F32),
            pltpu.VMEM((ITERS, 2, 8, 8, 4, 128), F32),
            pltpu.VMEM((5, 8, 4, 8, 4, 128), F32),
            pltpu.VMEM((16, 128), F32),
            pltpu.VMEM((16, 128), F32),
            dma((rows // CHUNK, 2)), dma((5,)),
            dma, dma, dma, dma,
            dma((ITERS,)), dma((ITERS,)),
            dma((ITERS,)), dma((ITERS, 2)), dma((ITERS,)), dma((ITERS,)),
            dma((5, 8)),
        ],
        compiler_params=pltpu.CompilerParams(
            collective_id=0, has_side_effects=True, vmem_limit_bytes=60 * 1024 * 1024
        ),
    )(
        reflect_re[0], reflect_im[0], focus_re[0].T, focus_im[0].T, first_arrival.T,
        jnp.asarray(t1), jnp.asarray(t2),
    )
    outs = pl.pallas_call(
        hand_on,
        out_shape=[jax.ShapeDtypeStruct((32, rows), F32)] * 4,
        in_specs=[vmem] * 4,
        out_specs=[vmem] * 4,
    )(*outs)
    return tuple(o.T[None] for o in outs)


def solution(mesh):
    placed = (
        P("freq", "row", None),
        P("freq", "row", None),
        P("freq", "row", None),
        P("freq", "row", None),
        P("row", None),
    )
    return jax.shard_map(
        local,
        mesh=mesh,
        in_specs=placed,
        out_specs=(P("freq", "row", None),) * 4,
        check_vma=False,
    )
```

```python
import functools
import math

import jax
import jax.numpy as jnp
import numpy as np
from jax import lax
from jax.experimental import pallas as pl
from jax.experimental.pallas import tpu as pltpu
from jax.sharding import PartitionSpec as P

MESH = pl.DeviceIdType.MESH
ITERS = 4
F32 = jnp.float32
BF16 = jnp.bfloat16
BLK = 216
CHUNK = 96


def split_np(table):
    hi = table.astype(jnp.bfloat16)
    lo = (table - hi.astype(np.float64)).astype(hi.dtype)
    return hi, lo


def tables():
    order = np.array(
        [
            x * 32 + z * 4 + y * 2 + c
            for z in range(8)
            for y in range(2)
            for c in range(2)
            for x in range(4)
        ]
    )
    t = np.arange(256)
    angle = 2.0 * math.pi * ((t[:, None] * order[None, :]) % 256) / 256
    weight = np.where(order == 0, 1.0 / 256, 2.0 / 256)
    t1 = np.concatenate([np.cos(angle) * weight, -np.sin(angle) * weight], axis=1)
    t2 = np.concatenate([np.cos(angle).T, -np.sin(angle).T], axis=0)
    out = []
    for table in (t1, t2):
        hi, lo = split_np(table)
        out.append(np.concatenate([hi, lo, hi], axis=1))
    return out


def split(v):
    hi = v.astype(BF16)
    lo = (v - hi.astype(F32)).astype(BF16)
    return hi, lo


def copies(src, dst, ssem, rsem, dev):
    return pltpu.make_async_remote_copy(
        src_ref=src, dst_ref=dst, send_sem=ssem, recv_sem=rsem, device_id=dev, device_id_type=MESH
    )


def wait_bytes(ref, sem):
    pltpu.make_async_copy(ref, ref, sem).wait()


def kernel(
    rre, rim, fre_h, fim_h, fa_h, t1_h, t2_h,
    mre, mim, pre, pim,
    stage, fbuf, fa, t1, t2, rcat, acc, fsend, gbuf, bsend, relay2, urecv, fasend, farecv,
    ld_sem, in_sem, ini_send, ini_recv, fa_send, fa_recv,
    f_send, f_recv, b1_send, b1_recv, b2_send, b2_send2, b2_recv,
):
    me = lax.axis_index("freq")
    row = lax.axis_index("row")
    x = me // 32
    z = (me // 4) % 8
    yh = (me // 2) % 2
    c = me % 2
    ypos = 2 * yh + row
    xs = [lax.rem(x + d, 4) for d in range(4)]
    zs = [lax.rem(z + d, 8) for d in range(8)]
    ys = [lax.rem(ypos + d, 4) for d in range(4)]
    cs = [c, 1 - c]

    xf, zf = [v * 32 for v in xs], [v * 4 for v in zs]

    def dev(xi, zi, yi, ci):
        return (xi * 32 + zi * 4 + (yi // 2) * 2 + ci, lax.rem(yi, 2))

    loads = [
        pltpu.make_async_copy(src, dst, in_sem.at[i])
        for i, (src, dst) in enumerate(
            ((fre_h, fbuf.at[0]), (fim_h, fbuf.at[1]), (fa_h, fa), (t1_h, t1), (t2_h, t2))
        )
    ]
    for load in loads:
        load.start()
    nchunk = rre.shape[0] // CHUNK
    for k in range(nchunk):
        for a, ref in enumerate((rre, rim)):
            pltpu.make_async_copy(
                ref.at[pl.ds(k * CHUNK, CHUNK)],
                stage.at[a, pl.ds(k * CHUNK, CHUNK)],
                ld_sem.at[k, a],
            ).start()

    xorder, zorder = (2, 1, 3, 0), (4, 3, 5, 2, 6, 1, 7)
    away = [
        (dx, dy, dz, dc) for dz in (*zorder, 0) for dx in xorder for dy in (1, 3) for dc in (1, 0)
    ]
    away += [(dx, dy, 0, dc) for dx in xorder for dy in (2, 0) for dc in (1, 0)][:-1]
    away += [(0, 0, dz, 0) for dz in zorder]
    barrier = pltpu.get_barrier_semaphore()
    for dx, dy, dz, dc in away:
        pl.semaphore_signal(
            barrier, inc=1, device_id=dev(xs[dx], zs[dz], ys[dy], cs[dc]), device_id_type=MESH
        )

    u2 = urecv.reshape(5 * 8 * 128, 128)
    for load in loads[:3]:
        load.wait()
    for q in range(4):
        base = (row * 4 + q) * 128
        for h in range(2):
            n = 128 if h == 0 else BLK - 128
            lo = BLK * q + 128 * h
            for ri in range(2):
                v = fbuf[ri, :, lo : lo + n]
                if n < 128:
                    v = jnp.concatenate([v, jnp.zeros((32, 128 - n), F32)], axis=1)
                u2[pl.ds(base + 2 * h + ri, 32, stride=4), :] = v
    myq = 2 * yh + c
    myp = x * 8 + z
    pick = lax.broadcasted_iota(jnp.int32, fa.shape, 0) == myp
    v = jnp.sum(jnp.where(pick, fa[...].astype(F32), 0.0), axis=0, keepdims=True)
    w = jnp.zeros((1, BLK), F32)
    for q in range(4):
        w = w + jnp.where(myq == q, v[:, BLK * q : BLK * q + BLK], 0.0)
    w = jnp.concatenate([w, jnp.zeros((1, 256 - BLK), F32)], axis=1)
    for h in range(2):
        fasend[8 * h : 8 * h + 8] = jnp.broadcast_to(w[:, 128 * h : 128 * h + 128], (8, 128))

    pl.semaphore_wait(barrier, len(away))
    partner = (me, 1 - row)
    mine = urecv.at[0, pl.ds(row * 4, 4)]
    ini = copies(mine, mine, ini_send, ini_recv, partner)
    ini.start()
    fac = copies(fasend, farecv, fa_send, fa_recv, partner)
    fac.start()

    def convert(k, carry):
        rows = pl.ds(pl.multiple_of(k * CHUNK, CHUNK), CHUNK)
        for a in range(2):
            wait_bytes(stage.at[a, pl.ds(0, CHUNK)], ld_sem.at[k, a])
            for b in range(8):
                v = stage[a, rows, BLK * b : BLK * b + BLK]
                v = jnp.concatenate([v, jnp.zeros((CHUNK, 256 - BLK), F32)], axis=1)
                hi, lo = split(v)
                rcat[b, rows, 512 * a : 512 * a + 256] = hi
                rcat[b, rows, 512 * a + 256 : 512 * a + 512] = lo
        return carry

    lax.fori_loop(0, nchunk, convert, 0)
    acc[864:, :] = jnp.zeros_like(acc[864:, :])
    fac.wait()
    for load in loads[3:]:
        load.wait()

    f1v = fsend.reshape(ITERS * 512, 128)
    g2 = gbuf.reshape(ITERS * 512, 128)
    bs2 = bsend.reshape(ITERS * 512, 128)
    ublk = urecv.reshape(5 * 32, 8, 4, 128)
    myn = (1 - row) * 4 + myq
    reach = jnp.concatenate([farecv[0:1], farecv[8:9]], axis=1)
    tid = lax.broadcasted_iota(jnp.int32, (256, 256), 0)
    dist = jnp.minimum(tid, 256 - tid).astype(F32)

    def apply(it, carry):
        sign = 1.0 - 2.0 * lax.rem(it, 2).astype(F32)
        extra = jnp.where(it == 2, 1.0, 0.0).astype(F32)

        def block(t, first):
            v = t // 2
            ci = lax.rem(c + 1 + jnp.where(it == 0, t, v), 2)
            y_own = 2 * (v % 2) + lax.rem(row + 1 + v // 2, 2)
            y_arr = 2 * lax.rem(yh + 1 + v // 2, 2) + lax.rem(row + 1 + t, 2)
            yi = jnp.where(it == 0, y_own, y_arr)
            n = (1 - lax.rem(yi, 2)) * 4 + (yi // 2) * 2 + ci

            @pl.when((it > 0) & (t < 7))
            def _():
                wait_bytes(urecv.at[it, n], b2_recv.at[it, n])

            @pl.when((it > 0) & (t == 7))
            def _():
                wait_bytes(urecv.at[it, n, pl.ds(0, 3)], b2_recv.at[it, n])

            @pl.when((it == 0) & (t == 4))
            def _():
                ini.wait()

            parts = []
            for ri in range(2):
                halves = []
                for h in range(2):
                    j = 2 * h + ri
                    now = u2[pl.ds((it * 8 + n) * 128 + j, 32, stride=4), :]
                    start = u2[pl.ds(n * 128 + j, 32, stride=4), :]
                    halves.append(now + extra * start)
                parts.append(jnp.concatenate(halves, axis=1))
            ur, ui = parts
            urh, url = split(ur)
            uih, uil = split(ui)
            sg = sign.astype(BF16)
            w1 = jnp.concatenate([urh, uih, url, uil], axis=0)
            w2 = jnp.concatenate([-(sg * uih), sg * urh, -(sg * uil), sg * url], axis=0)
            w = jnp.concatenate([w1, w1, w2, w2], axis=1)
            part = lax.dot_general(
                rcat[n], w, (((1,), (1,)), ((), ())), preferred_element_type=F32
            )
            if first:
                acc[0:864, :] = part
            else:
                acc[0:864, :] += part

        block(jnp.int32(0), True)

        def rest(t, carry):
            block(t, False)
            return carry

        lax.fori_loop(1, 8, rest, 0)

        for dy in (1, 3):
            yi = ys[dy]
            for cd in range(2):
                base, par = (yi // 2) * 2 + cd, lax.rem(yi, 2)
                q = base
                for h in range(2):
                    v = acc[pl.ds(pl.multiple_of(BLK * q + 128 * h, 8), 128), :].T
                    v = v[0:64] + v[64:128]
                    for ri in range(2):
                        f1v[pl.ds(it * 512 + q * 128 + 2 * h + ri, 32, stride=4), :] = v[
                            32 * ri : 32 * ri + 32
                        ]
                for dz in (*zorder, 0):
                    for dx in xorder:
                        copies(
                            fsend.at[it, q, xs[dx], zs[dz]],
                            gbuf.at[it, z, yh, c, x],
                            f_send.at[it],
                            f_recv.at[it],
                            (xf[dx] + (zf[dz] + base), par),
                        ).start()
        wait_bytes(gbuf.at[it], f_recv.at[it])

        g = jnp.concatenate(
            [
                jnp.concatenate(
                    [g2[pl.ds(it * 512 + 2 * h + ri, 128, stride=4), :] for h in range(2)], axis=1
                )
                for ri in range(2)
            ],
            axis=0,
        )
        gh, gl = split(g)
        tr = jnp.dot(t1[...], jnp.concatenate([gh, gh, gl], axis=0), preferred_element_type=F32)
        tr = jnp.where(dist < reach, tr, 0.0)
        th, tl = split(tr)
        out = jnp.dot(t2[...], jnp.concatenate([th, th, tl], axis=0), preferred_element_type=F32)
        for h in range(2):
            for ri in range(2):
                bs2[pl.ds(it * 512 + 2 * h + ri, 128, stride=4), :] = out[
                    128 * ri : 128 * ri + 128, 128 * h : 128 * h + 128
                ]
        parts = ((1 - yh, 1 - c), (1 - yh, c), (yh, 1 - c), (yh, c))
        for i, (v, cc) in enumerate(parts):
            for dz in zorder:
                copies(
                    bsend.at[it, zs[dz], v, cc],
                    relay2.at[it, v, cc, z],
                    b1_send.at[it],
                    b1_recv.at[it, i],
                    dev(x, zs[dz], ypos, c),
                ).start()
            relay2[it, v, cc, z] = bsend[it, z, v, cc]

        def out_to(dx, v, cc, r, sem):
            copies(
                relay2.at[it, v, cc, :, xs[dx]],
                urecv.at[it + 1, myn, x],
                sem,
                b2_recv.at[it + 1, myn],
                dev(xs[dx], z, 2 * v + r, cc),
            ).start()

        for i, (v, cc) in enumerate(parts):
            wait_bytes(relay2.at[it, v, cc, pl.ds(0, 7)], b1_recv.at[it, i])
            for dx in xorder:
                out_to(dx, v, cc, 1 - row, b2_send.at[it])

            @pl.when(it < ITERS - 1)
            def _():
                for dx in xorder:
                    if i == 3 and dx == 0:
                        urecv[it + 1, myn, x] = relay2[it, v, cc, :, x]
                    else:
                        out_to(dx, v, cc, row, b2_send2.at[it])

        return carry

    lax.fori_loop(0, ITERS, apply, 0)

    def result(slot, outs):
        for q in range(4):
            n = row * 4 + q
            if slot == ITERS:
                wait_bytes(urecv.at[ITERS, n], b2_recv.at[ITERS, n])
            for h in range(2):
                m = 128 if h == 0 else BLK - 128
                lo = BLK * q + 128 * h
                for ri in range(2):
                    j = 2 * h + ri
                    v = u2[pl.ds((slot * 8 + n) * 128 + j, 32, stride=4), :]
                    if slot == ITERS:
                        v = v + u2[pl.ds(n * 128 + j, 32, stride=4), :]
                    outs[ri][:, lo : lo + m] = v[:, 0:m]

    result(ITERS - 1, (mre, mim))
    for it in range(ITERS):
        wait_bytes(fsend.at[it], f_send.at[it])
        wait_bytes(gbuf.at[it, pl.ds(0, 7)], b1_send.at[it])
        wait_bytes(ublk.at[pl.ds(0, 16)], b2_send.at[it])
        if it < ITERS - 1:
            wait_bytes(ublk.at[pl.ds(0, 15)], b2_send2.at[it])
    result(ITERS, (pre, pim))


def hand_on(*refs):
    for i in range(4):
        refs[4 + i][...] = refs[i][...]


def local(reflect_re, reflect_im, focus_re, focus_im, first_arrival):
    rows, cols = reflect_re.shape[1:]
    t1, t2 = tables()
    vmem = pl.BlockSpec(memory_space=pltpu.VMEM)
    hbm = pl.BlockSpec(memory_space=pl.ANY)
    dma = pltpu.SemaphoreType.DMA
    outs = pl.pallas_call(
        kernel,
        out_shape=[jax.ShapeDtypeStruct((32, rows), F32)] * 4,
        in_specs=[hbm] * 7,
        out_specs=[vmem] * 4,
        scratch_shapes=[
            pltpu.VMEM((2, rows, cols), F32),
            pltpu.VMEM((2, 32, rows), F32),
            pltpu.VMEM((32, rows), jnp.int32),
            pltpu.VMEM(t1.shape, BF16),
            pltpu.VMEM(t2.shape, BF16),
            pltpu.VMEM((8, rows, 1024), BF16),
            pltpu.VMEM((rows + 48, 128), F32),
            pltpu.VMEM((ITERS, 4, 4, 8, 4, 128), F32),
            pltpu.VMEM((ITERS, 8, 2, 2, 4, 4, 128), F32),
            pltpu.VMEM((ITERS, 8, 2, 2, 4, 4, 128), F32),
            pltpu.VMEM((ITERS, 2, 2, 8, 4, 4, 128), F32),
            pltpu.VMEM((5, 8, 4, 8, 4, 128), F32),
            pltpu.VMEM((16, 128), F32),
            pltpu.VMEM((16, 128), F32),
            dma((rows // CHUNK, 2)), dma((5,)),
            dma, dma, dma, dma,
            dma((ITERS,)), dma((ITERS,)),
            dma((ITERS,)), dma((ITERS, 4)), dma((ITERS,)), dma((ITERS,)),
            dma((5, 8)),
        ],
        compiler_params=pltpu.CompilerParams(
            collective_id=0, has_side_effects=True, vmem_limit_bytes=60 * 1024 * 1024
        ),
    )(
        reflect_re[0], reflect_im[0], focus_re[0].T, focus_im[0].T, first_arrival.T,
        jnp.asarray(t1), jnp.asarray(t2),
    )
    outs = pl.pallas_call(
        hand_on,
        out_shape=[jax.ShapeDtypeStruct((32, rows), F32)] * 4,
        in_specs=[vmem] * 4,
        out_specs=[vmem] * 4,
    )(*outs)
    return tuple(o.T[None] for o in outs)


def solution(mesh):
    placed = (
        P("freq", "row", None),
        P("freq", "row", None),
        P("freq", "row", None),
        P("freq", "row", None),
        P("row", None),
    )
    return jax.shard_map(
        local,
        mesh=mesh,
        in_specs=placed,
        out_specs=(P("freq", "row", None),) * 4,
        check_vma=False,
    )
```

```python
import functools
import math

import jax
import jax.numpy as jnp
import numpy as np
from jax import lax
from jax.experimental import pallas as pl
from jax.experimental.pallas import tpu as pltpu
from jax.sharding import PartitionSpec as P

MESH = pl.DeviceIdType.MESH
ITERS = 4
F32 = jnp.float32
BF16 = jnp.bfloat16
BLK = 216
CHUNK = 96


def split_np(table):
    hi = table.astype(jnp.bfloat16)
    lo = (table - hi.astype(np.float64)).astype(hi.dtype)
    return hi, lo


def tables():
    order = np.array(
        [
            x * 32 + z * 4 + y * 2 + c
            for z in range(8)
            for y in range(2)
            for c in range(2)
            for x in range(4)
        ]
    )
    t = np.arange(256)
    angle = 2.0 * math.pi * ((t[:, None] * order[None, :]) % 256) / 256
    weight = np.where(order == 0, 1.0 / 256, 2.0 / 256)
    t1 = np.concatenate([np.cos(angle) * weight, -np.sin(angle) * weight], axis=1)
    t2 = np.concatenate([np.cos(angle).T, -np.sin(angle).T], axis=0)
    out = []
    for table in (t1, t2):
        hi, lo = split_np(table)
        out.append(np.concatenate([hi, lo, hi], axis=1))
    return out


def split(v):
    hi = v.astype(BF16)
    lo = (v - hi.astype(F32)).astype(BF16)
    return hi, lo


def copies(src, dst, ssem, rsem, dev):
    return pltpu.make_async_remote_copy(
        src_ref=src, dst_ref=dst, send_sem=ssem, recv_sem=rsem, device_id=dev, device_id_type=MESH
    )


def wait_bytes(ref, sem):
    pltpu.make_async_copy(ref, ref, sem).wait()


def kernel(
    rre, rim, fre_h, fim_h, fa_h, t1_h, t2_h,
    mre, mim, pre, pim,
    stage, fbuf, fa, t1, t2, rcat, acc, fsend, gbuf, bsend, relay2, urecv, fasend, farecv,
    ld_sem, in_sem, ini_send, ini_recv, fa_send, fa_recv,
    f_send, f_recv, b1_send, b1_recv, b2_send, b2_send2, b2_recv,
):
    me = lax.axis_index("freq")
    row = lax.axis_index("row")
    x = me // 32
    z = (me // 4) % 8
    yh = (me // 2) % 2
    c = me % 2
    ypos = 2 * yh + row
    xs = [lax.rem(x + d, 4) for d in range(4)]
    zs = [lax.rem(z + d, 8) for d in range(8)]
    ys = [lax.rem(ypos + d, 4) for d in range(4)]
    cs = [c, 1 - c]

    xf, zf = [v * 32 for v in xs], [v * 4 for v in zs]

    def dev(xi, zi, yi, ci):
        return (xi * 32 + zi * 4 + (yi // 2) * 2 + ci, lax.rem(yi, 2))

    loads = [
        pltpu.make_async_copy(src, dst, in_sem.at[i])
        for i, (src, dst) in enumerate(
            ((fre_h, fbuf.at[0]), (fim_h, fbuf.at[1]), (fa_h, fa), (t1_h, t1), (t2_h, t2))
        )
    ]
    for load in loads:
        load.start()
    nchunk = rre.shape[0] // CHUNK
    for k in range(nchunk):
        for a, ref in enumerate((rre, rim)):
            pltpu.make_async_copy(
                ref.at[pl.ds(k * CHUNK, CHUNK)],
                stage.at[a, pl.ds(k * CHUNK, CHUNK)],
                ld_sem.at[k, a],
            ).start()

    xorder, zorder = (2, 1, 3, 0), (4, 3, 5, 2, 6, 1, 7)
    away = [
        (dx, dy, dz, dc) for dz in (*zorder, 0) for dx in xorder for dy in (1, 3) for dc in (1, 0)
    ]
    away += [(dx, dy, 0, dc) for dx in xorder for dy in (2, 0) for dc in (1, 0)][:-1]
    away += [(0, 0, dz, 0) for dz in zorder]
    barrier = pltpu.get_barrier_semaphore()
    for dx, dy, dz, dc in away:
        pl.semaphore_signal(
            barrier, inc=1, device_id=dev(xs[dx], zs[dz], ys[dy], cs[dc]), device_id_type=MESH
        )

    u2 = urecv.reshape(5 * 8 * 128, 128)
    for load in loads[:3]:
        load.wait()
    for q in range(4):
        base = (row * 4 + q) * 128
        for h in range(2):
            n = 128 if h == 0 else BLK - 128
            lo = BLK * q + 128 * h
            for ri in range(2):
                v = fbuf[ri, :, lo : lo + n]
                if n < 128:
                    v = jnp.concatenate([v, jnp.zeros((32, 128 - n), F32)], axis=1)
                u2[pl.ds(base + 2 * h + ri, 32, stride=4), :] = v
    myq = 2 * yh + c
    myp = x * 8 + z
    pick = lax.broadcasted_iota(jnp.int32, fa.shape, 0) == myp
    v = jnp.sum(jnp.where(pick, fa[...].astype(F32), 0.0), axis=0, keepdims=True)
    w = jnp.zeros((1, BLK), F32)
    for q in range(4):
        w = w + jnp.where(myq == q, v[:, BLK * q : BLK * q + BLK], 0.0)
    w = jnp.concatenate([w, jnp.zeros((1, 256 - BLK), F32)], axis=1)
    for h in range(2):
        fasend[8 * h : 8 * h + 8] = jnp.broadcast_to(w[:, 128 * h : 128 * h + 128], (8, 128))

    pl.semaphore_wait(barrier, len(away))
    partner = (me, 1 - row)
    for q in (1 - c, c, 3 - c, 2 + c):
        mine = urecv.at[0, row * 4 + q]
        copies(mine, mine, ini_send, ini_recv.at[q], partner).start()
    fac = copies(fasend, farecv, fa_send, fa_recv, partner)
    fac.start()

    def convert(k, carry):
        rows = pl.ds(pl.multiple_of(k * CHUNK, CHUNK), CHUNK)
        for a in range(2):
            wait_bytes(stage.at[a, pl.ds(0, CHUNK)], ld_sem.at[k, a])
            for b in range(8):
                v = stage[a, rows, BLK * b : BLK * b + BLK]
                v = jnp.concatenate([v, jnp.zeros((CHUNK, 256 - BLK), F32)], axis=1)
                hi, lo = split(v)
                rcat[b, rows, 512 * a : 512 * a + 256] = hi
                rcat[b, rows, 512 * a + 256 : 512 * a + 512] = lo
        return carry

    lax.fori_loop(0, nchunk, convert, 0)
    acc[864:, :] = jnp.zeros_like(acc[864:, :])
    fac.wait()
    for load in loads[3:]:
        load.wait()

    f1v = fsend.reshape(ITERS * 512, 128)
    g2 = gbuf.reshape(ITERS * 512, 128)
    bs2 = bsend.reshape(ITERS * 512, 128)
    ublk = urecv.reshape(5 * 32, 8, 4, 128)
    myn = (1 - row) * 4 + myq
    reach = jnp.concatenate([farecv[0:1], farecv[8:9]], axis=1)
    tid = lax.broadcasted_iota(jnp.int32, (256, 256), 0)
    dist = jnp.minimum(tid, 256 - tid).astype(F32)

    def apply(it, carry):
        sign = 1.0 - 2.0 * lax.rem(it, 2).astype(F32)
        extra = jnp.where(it == 2, 1.0, 0.0).astype(F32)

        def block(t, first):
            v = t // 2
            ci = lax.rem(c + 1 + jnp.where(it == 0, t, v), 2)
            y_own = 2 * (v % 2) + lax.rem(row + 1 + v // 2, 2)
            y_arr = 2 * lax.rem(yh + 1 + v // 2, 2) + lax.rem(row + 1 + t, 2)
            yi = jnp.where(it == 0, y_own, y_arr)
            n = (1 - lax.rem(yi, 2)) * 4 + (yi // 2) * 2 + ci

            @pl.when((it > 0) & (t < 7))
            def _():
                wait_bytes(urecv.at[it, n], b2_recv.at[it, n])

            @pl.when((it > 0) & (t == 7))
            def _():
                wait_bytes(urecv.at[it, n, pl.ds(0, 3)], b2_recv.at[it, n])

            @pl.when((it == 0) & (t >= 4))
            def _():
                wait_bytes(urecv.at[0, n], ini_recv.at[(yi // 2) * 2 + ci])

            parts = []
            for ri in range(2):
                halves = []
                for h in range(2):
                    j = 2 * h + ri
                    now = u2[pl.ds((it * 8 + n) * 128 + j, 32, stride=4), :]
                    start = u2[pl.ds(n * 128 + j, 32, stride=4), :]
                    halves.append(now + extra * start)
                parts.append(jnp.concatenate(halves, axis=1))
            ur, ui = parts
            urh, url = split(ur)
            uih, uil = split(ui)
            sg = sign.astype(BF16)
            w1 = jnp.concatenate([urh, uih, url, uil], axis=0)
            w2 = jnp.concatenate([-(sg * uih), sg * urh, -(sg * uil), sg * url], axis=0)
            w = jnp.concatenate([w1, w1, w2, w2], axis=1)
            part = lax.dot_general(
                rcat[n], w, (((1,), (1,)), ((), ())), preferred_element_type=F32
            )
            if first:
                acc[0:864, :] = part
            else:
                acc[0:864, :] += part

        block(jnp.int32(0), True)

        def rest(t, carry):
            block(t, False)
            return carry

        lax.fori_loop(1, 8, rest, 0)

        for dy in (1, 3):
            yi = ys[dy]
            for cd in range(2):
                base, par = (yi // 2) * 2 + cd, lax.rem(yi, 2)
                q = base
                for h in range(2):
                    v = acc[pl.ds(pl.multiple_of(BLK * q + 128 * h, 8), 128), :].T
                    v = v[0:64] + v[64:128]
                    for ri in range(2):
                        f1v[pl.ds(it * 512 + q * 128 + 2 * h + ri, 32, stride=4), :] = v[
                            32 * ri : 32 * ri + 32
                        ]
                for dz in (*zorder, 0):
                    for dx in xorder:
                        copies(
                            fsend.at[it, q, xs[dx], zs[dz]],
                            gbuf.at[it, z, yh, c, x],
                            f_send.at[it],
                            f_recv.at[it],
                            (xf[dx] + (zf[dz] + base), par),
                        ).start()
        wait_bytes(gbuf.at[it], f_recv.at[it])

        g = jnp.concatenate(
            [
                jnp.concatenate(
                    [g2[pl.ds(it * 512 + 2 * h + ri, 128, stride=4), :] for h in range(2)], axis=1
                )
                for ri in range(2)
            ],
            axis=0,
        )
        gh, gl = split(g)
        tr = jnp.dot(t1[...], jnp.concatenate([gh, gh, gl], axis=0), preferred_element_type=F32)
        tr = jnp.where(dist < reach, tr, 0.0)
        th, tl = split(tr)
        out = jnp.dot(t2[...], jnp.concatenate([th, th, tl], axis=0), preferred_element_type=F32)
        for h in range(2):
            for ri in range(2):
                bs2[pl.ds(it * 512 + 2 * h + ri, 128, stride=4), :] = out[
                    128 * ri : 128 * ri + 128, 128 * h : 128 * h + 128
                ]
        parts = ((1 - yh, 1 - c), (1 - yh, c), (yh, 1 - c), (yh, c))
        for i, (v, cc) in enumerate(parts):
            for dz in zorder:
                copies(
                    bsend.at[it, zs[dz], v, cc],
                    relay2.at[it, v, cc, z],
                    b1_send.at[it],
                    b1_recv.at[it, i],
                    dev(x, zs[dz], ypos, c),
                ).start()
            relay2[it, v, cc, z] = bsend[it, z, v, cc]

        def out_to(dx, v, cc, r, sem):
            copies(
                relay2.at[it, v, cc, :, xs[dx]],
                urecv.at[it + 1, myn, x],
                sem,
                b2_recv.at[it + 1, myn],
                dev(xs[dx], z, 2 * v + r, cc),
            ).start()

        for i, (v, cc) in enumerate(parts):
            wait_bytes(relay2.at[it, v, cc, pl.ds(0, 7)], b1_recv.at[it, i])
            for dx in xorder:
                out_to(dx, v, cc, 1 - row, b2_send.at[it])

            @pl.when(it < ITERS - 1)
            def _():
                for dx in xorder:
                    if i == 3 and dx == 0:
                        urecv[it + 1, myn, x] = relay2[it, v, cc, :, x]
                    else:
                        out_to(dx, v, cc, row, b2_send2.at[it])

        return carry

    lax.fori_loop(0, ITERS, apply, 0)

    def result(slot, outs):
        for q in range(4):
            n = row * 4 + q
            if slot == ITERS:
                wait_bytes(urecv.at[ITERS, n], b2_recv.at[ITERS, n])
            for h in range(2):
                m = 128 if h == 0 else BLK - 128
                lo = BLK * q + 128 * h
                for ri in range(2):
                    j = 2 * h + ri
                    v = u2[pl.ds((slot * 8 + n) * 128 + j, 32, stride=4), :]
                    if slot == ITERS:
                        v = v + u2[pl.ds(n * 128 + j, 32, stride=4), :]
                    outs[ri][:, lo : lo + m] = v[:, 0:m]

    result(ITERS - 1, (mre, mim))
    wait_bytes(urecv.at[0, pl.ds(0, 4)], ini_send)
    for it in range(ITERS):
        wait_bytes(fsend.at[it], f_send.at[it])
        wait_bytes(gbuf.at[it, pl.ds(0, 7)], b1_send.at[it])
        wait_bytes(ublk.at[pl.ds(0, 16)], b2_send.at[it])
        if it < ITERS - 1:
            wait_bytes(ublk.at[pl.ds(0, 15)], b2_send2.at[it])
    result(ITERS, (pre, pim))


def hand_on(*refs):
    for i in range(4):
        refs[4 + i][...] = refs[i][...]


def local(reflect_re, reflect_im, focus_re, focus_im, first_arrival):
    rows, cols = reflect_re.shape[1:]
    t1, t2 = tables()
    vmem = pl.BlockSpec(memory_space=pltpu.VMEM)
    hbm = pl.BlockSpec(memory_space=pl.ANY)
    dma = pltpu.SemaphoreType.DMA
    outs = pl.pallas_call(
        kernel,
        out_shape=[jax.ShapeDtypeStruct((32, rows), F32)] * 4,
        in_specs=[hbm] * 7,
        out_specs=[vmem] * 4,
        scratch_shapes=[
            pltpu.VMEM((2, rows, cols), F32),
            pltpu.VMEM((2, 32, rows), F32),
            pltpu.VMEM((32, rows), jnp.int32),
            pltpu.VMEM(t1.shape, BF16),
            pltpu.VMEM(t2.shape, BF16),
            pltpu.VMEM((8, rows, 1024), BF16),
            pltpu.VMEM((rows + 48, 128), F32),
            pltpu.VMEM((ITERS, 4, 4, 8, 4, 128), F32),
            pltpu.VMEM((ITERS, 8, 2, 2, 4, 4, 128), F32),
            pltpu.VMEM((ITERS, 8, 2, 2, 4, 4, 128), F32),
            pltpu.VMEM((ITERS, 2, 2, 8, 4, 4, 128), F32),
            pltpu.VMEM((5, 8, 4, 8, 4, 128), F32),
            pltpu.VMEM((16, 128), F32),
            pltpu.VMEM((16, 128), F32),
            dma((rows // CHUNK, 2)), dma((5,)),
            dma, dma((4,)), dma, dma,
            dma((ITERS,)), dma((ITERS,)),
            dma((ITERS,)), dma((ITERS, 4)), dma((ITERS,)), dma((ITERS,)),
            dma((5, 8)),
        ],
        compiler_params=pltpu.CompilerParams(
            collective_id=0, has_side_effects=True, vmem_limit_bytes=60 * 1024 * 1024
        ),
    )(
        reflect_re[0], reflect_im[0], focus_re[0].T, focus_im[0].T, first_arrival.T,
        jnp.asarray(t1), jnp.asarray(t2),
    )
    outs = pl.pallas_call(
        hand_on,
        out_shape=[jax.ShapeDtypeStruct((32, rows), F32)] * 4,
        in_specs=[vmem] * 4,
        out_specs=[vmem] * 4,
    )(*outs)
    return tuple(o.T[None] for o in outs)


def solution(mesh):
    placed = (
        P("freq", "row", None),
        P("freq", "row", None),
        P("freq", "row", None),
        P("freq", "row", None),
        P("row", None),
    )
    return jax.shard_map(
        local,
        mesh=mesh,
        in_specs=placed,
        out_specs=(P("freq", "row", None),) * 4,
        check_vma=False,
    )
```
